32 devices in a mesh: wide: 4 (over x, core), narrow: 8 (over z, y).
Axes of the slice: x: 2, y: 2, z: 4, core: 2. Of those that a mesh axis runs over, the one named last changes fastest.
Arguments:
- velocity: float32 [3, 1, 4096, 4096], P(None, None, ('wide', 'narrow')), may hold values from -6 to 6
- plane_wavenumber: float32 [1], replicated, may hold values from 2 to 1024
Outputs:
- projected: float32 [3, 1, 4096, 4096], P(None, None, ('wide', 'narrow'))
The draws below stay inside these ranges and needn't reach their ends.
All inputs are finite; a program needn't handle non-finite values.
Results may differ from the reference program's by a relative error of at most 0.00007.
Values sent between devices are 32-bit elements; how exact they have to be, the bound alone decides.
No kernel may reach another device: no remote copies, remote signals or barrier semaphores. Data moves between devices by JAX's collectives and lax.ppermute only.
A program may use at most 128 MiB of HBM per device.

```python
import math
import jax
import jax.numpy as jnp

NX = 4096
NY = 4096
PLANES = 1


def block_scale(rng, dims, cuts, least, high):
    factor_of = 1.0
    for position, shards_of in cuts:
        heights = jax.random.uniform(jax.random.fold_in(jax.random.fold_in(rng, 6), position), (shards_of,), jnp.float32, least / len(cuts), high / len(cuts))
        factor_of = factor_of * jnp.repeat(jnp.exp(heights), dims[position] // shards_of).reshape((-1,) + (1,) * (len(dims) - 1 - position))
    return factor_of


def centred(rng, dims, scale, reach, split=(), dtype=jnp.bfloat16):
    values = scale * jax.random.normal(rng, dims, jnp.float32)
    if split:
        values = values * block_scale(rng, dims, split, -0.22, 0.18)
    return jnp.clip(values, -reach, reach).astype(dtype)


def setup_inputs(seed: int = 0) -> dict:
    key_list = jax.random.split(jax.random.key(seed), 3)
    return {
        "velocity": centred(key_list[0], (3, PLANES, NY, NX), 1.0, 6.0, ((2, 32),), jnp.float32),
        "plane_wavenumber": jnp.clip(jnp.exp(jax.random.uniform(key_list[1], (PLANES,), jnp.float32, math.log(2.0), math.log(1024.0))), 2.0, 1024.0),
    }


def reference(velocity, plane_wavenumber):
    keep_x = NX // 3 + 1
    spectrum = jnp.fft.rfft(velocity, axis=3)[..., :keep_x]
    spectrum = jnp.fft.fft(spectrum, axis=2)
    index_y = jnp.arange(NY)
    signed_y = jnp.where(index_y <= NY // 2, index_y, index_y - NY)
    retained = (jnp.abs(signed_y) <= NY // 3).astype(jnp.float32)[None, :, None]
    wave_x = jnp.arange(keep_x).astype(jnp.float32)[None, None, :]
    wave_y = signed_y.astype(jnp.float32)[None, :, None]
    wave_z = plane_wavenumber[:, None, None]
    wave_square = wave_x * wave_x + wave_y * wave_y + wave_z * wave_z
    waves = (wave_x, wave_y, wave_z)
    divergence = wave_x * spectrum[0] + wave_y * spectrum[1] + wave_z * spectrum[2]
    solenoidal = jnp.stack([(spectrum[component] - waves[component] * divergence / wave_square) * retained for component in range(3)])
    returned = jnp.fft.ifft(solenoidal, axis=2)
    padded = jnp.pad(returned, ((0, 0), (0, 0), (0, 0), (0, NX // 2 + 1 - keep_x)))
    return jnp.fft.irfft(padded, n=NX, axis=3).astype(jnp.float32)
```

```python
import math

import jax
import jax.numpy as jnp
import numpy as np
from jax import lax
from jax.experimental import pallas as pl
from jax.experimental.pallas import tpu as pltpu
from jax.sharding import PartitionSpec as P

radix_split = 64
highest = lax.Precision.HIGHEST


def angle_tables(row_size, col_size, period, direction):
    product = jnp.arange(row_size)[:, None] * jnp.arange(col_size)[None, :] % period
    angles = direction * 2.0 * math.pi * product.astype(jnp.float32) / period
    return (jnp.cos(angles), jnp.sin(angles))


def complex_product(pattern, left_real, left_imag, table_real, table_imag):
    out_real = jnp.einsum(pattern, left_real, table_real, precision=highest) - jnp.einsum(
        pattern, left_imag, table_imag, precision=highest
    )
    out_imag = jnp.einsum(pattern, left_real, table_imag, precision=highest) + jnp.einsum(
        pattern, left_imag, table_real, precision=highest
    )
    return (out_real, out_imag)


def transform(real_part, imag_part, direction):
    length = real_part.shape[-1]
    inner_size = length // radix_split
    leading = real_part.shape[:-1]
    grid_real = real_part.reshape(leading + (radix_split, inner_size))
    grid_imag = imag_part.reshape(leading + (radix_split, inner_size))
    outer_cos, outer_sin = angle_tables(radix_split, radix_split, radix_split, direction)
    section_real, section_imag = complex_product(
        "...ab,ak->...kb", grid_real, grid_imag, outer_cos, outer_sin
    )
    twist_cos, twist_sin = angle_tables(radix_split, inner_size, length, direction)
    turned_real = section_real * twist_cos - section_imag * twist_sin
    turned_imag = section_real * twist_sin + section_imag * twist_cos
    inner_cos, inner_sin = angle_tables(inner_size, inner_size, inner_size, direction)
    final_real, final_imag = complex_product(
        "...kb,bm->...mk", turned_real, turned_imag, inner_cos, inner_sin
    )
    return (final_real.reshape(leading + (length,)), final_imag.reshape(leading + (length,)))


def project(lines, wave_x, wave_z, kept_line):
    groups, per_device, length_y = lines.shape
    shaped = lines.reshape(3, 2, groups // 6, per_device, length_y)
    spec_real, spec_imag = transform(shaped[:, 0], shaped[:, 1], -1.0)
    index_y = jnp.arange(length_y)
    signed_y = jnp.where(index_y <= length_y // 2, index_y, index_y - length_y)
    kept_y = jnp.abs(signed_y) <= length_y // 3
    retained = (kept_line & kept_y[None, None, :]).astype(jnp.float32)
    wave_y = signed_y.astype(jnp.float32)[None, None, :]
    wave_square = wave_x * wave_x + wave_y * wave_y + wave_z * wave_z
    waves = (wave_x, wave_y, wave_z)
    div_real = wave_x * spec_real[0] + wave_y * spec_real[1] + wave_z * spec_real[2]
    div_imag = wave_x * spec_imag[0] + wave_y * spec_imag[1] + wave_z * spec_imag[2]
    proj_real = jnp.stack(
        [
            (spec_real[component] - waves[component] * div_real / wave_square) * retained
            for component in range(3)
        ]
    )
    proj_imag = jnp.stack(
        [
            (spec_imag[component] - waves[component] * div_imag / wave_square) * retained
            for component in range(3)
        ]
    )
    back_real, back_imag = transform(proj_real, proj_imag, 1.0)
    return jnp.stack([back_real / length_y, back_imag / length_y], axis=1).reshape(
        groups, per_device, length_y
    )


def first_send(spectrum, first_size):
    groups, rows, span = spectrum.shape
    return (
        spectrum.reshape(groups, rows, first_size, span // first_size)
        .transpose(2, 0, 1, 3)
        .reshape(first_size, 1, -1)
    )


def second_send(received, first_size, second_size, groups, rows, per_device):
    shaped = received.reshape(first_size, groups, rows, second_size, per_device)
    return shaped.transpose(3, 1, 4, 0, 2).reshape(second_size, 1, -1)


def arrange_lines(received, first_size, second_size, groups, rows, per_device):
    shaped = received.reshape(second_size, groups, per_device, first_size, rows)
    ordered = shaped.transpose(1, 2, 0, 3, 4)
    return ordered.reshape(groups, per_device, -1)


def first_return(solved, first_size, second_size, rows):
    groups, per_device, _ = solved.shape
    shaped = solved.reshape(groups, per_device, second_size, first_size, rows).transpose(
        2, 0, 1, 3, 4
    )
    return shaped.reshape(second_size, 1, -1)


def second_return(received, first_size, second_size, groups, rows, per_device):
    shaped = received.reshape(second_size, groups, per_device, first_size, rows)
    return shaped.transpose(3, 1, 4, 0, 2).reshape(first_size, 1, -1)


def arrange_rows(received, first_size, groups, rows):
    shaped = received.reshape(first_size, groups, rows, -1)
    return shaped.transpose(1, 2, 0, 3).reshape(groups, rows, -1)


def local_generic(velocity, plane_wavenumber):
    components, plane_count, row_count, x_length = velocity.shape
    wide_size = lax.axis_size("wide")
    narrow_size = lax.axis_size("narrow")
    device_count = wide_size * narrow_size
    keep_x = x_length // 3 + 1
    spec_real, spec_imag = transform(velocity, jnp.zeros_like(velocity), -1.0)
    spec_real = spec_real[..., :keep_x]
    spec_imag = spec_imag[..., :keep_x]
    per_device = (keep_x + device_count - 1) // device_count
    line_span = per_device * device_count
    gap = ((0, 0), (0, 0), (0, 0), (0, 0), (0, line_span - keep_x))
    stacked = jnp.stack([spec_real, spec_imag], axis=1)
    spectrum = jnp.pad(stacked, gap).reshape(components * 2 * plane_count, row_count, line_span)
    groups = spectrum.shape[0]
    halfway = lax.all_to_all(
        first_send(spectrum, narrow_size), "narrow", split_axis=0, concat_axis=1, tiled=True
    )
    outgoing = second_send(halfway, narrow_size, wide_size, groups, row_count, per_device)
    arrived = lax.all_to_all(outgoing, "wide", split_axis=0, concat_axis=1, tiled=True)
    lines = arrange_lines(arrived, narrow_size, wide_size, groups, row_count, per_device)
    line_start = (
        lax.axis_index("narrow") * (per_device * wide_size) + lax.axis_index("wide") * per_device
    )
    indices = line_start + jnp.arange(per_device)
    wave_x = indices.astype(jnp.float32)[None, :, None]
    wave_z = plane_wavenumber[:, None, None]
    kept_line = (indices < keep_x)[None, :, None]
    solved = project(lines, wave_x, wave_z, kept_line)
    halfway = lax.all_to_all(
        first_return(solved, narrow_size, wide_size, row_count),
        "wide",
        split_axis=0,
        concat_axis=1,
        tiled=True,
    )
    outgoing = second_return(halfway, narrow_size, wide_size, groups, row_count, per_device)
    arrived = lax.all_to_all(outgoing, "narrow", split_axis=0, concat_axis=1, tiled=True)
    returned = arrange_rows(arrived, narrow_size, groups, row_count)
    columns = returned.reshape(components, 2, plane_count, row_count, line_span)[..., :keep_x]
    weights = jnp.where(jnp.arange(keep_x) == 0, 1.0, 2.0).astype(jnp.float32)
    widen = ((0, 0), (0, 0), (0, 0), (0, x_length - keep_x))
    back_real = jnp.pad(columns[:, 0] * weights, widen)
    back_imag = jnp.pad(columns[:, 1] * weights, widen)
    out_real, out_imag = transform(back_real, back_imag, 1.0)
    return out_real / x_length


radix = 16
lane = 128
tile = 8
axes = ("wide", "narrow")


def split_parts(values):
    high = values.astype(jnp.bfloat16)
    low = (values - high.astype(jnp.float32)).astype(jnp.bfloat16)
    return high, low


def split_table(values):
    values = values.astype(np.float32)
    high = values.astype(jnp.bfloat16)
    low = (values - high.astype(np.float32)).astype(jnp.bfloat16)
    return high, low


def turns(product, period):
    angle = 2.0 * np.pi * (np.asarray(product) % period) / period
    return np.cos(angle), np.sin(angle)


def twist_table(inner):
    return turns(np.arange(radix)[:, None] * np.arange(inner)[None, :], radix * inner)


def line_slots(per_device):
    main = per_device // tile * tile
    half = tile // 2
    slots = [(line, line, 0) for line in range(main)]
    slots += [(main + line, line, 1) for line in range(main)]
    for extra in range(per_device - main):
        slots.append((2 * main + extra, main + extra, 0))
        slots.append((2 * main + half + extra, main + extra, 1))
    return slots


def row_table(inner, per_device, shares, block):
    rows = np.zeros((2 * shares * block, 2 * inner))
    points = np.arange(inner)
    for share in range(shares):
        for row, line, part in line_slots(per_device):
            q = share * per_device + line
            cos, sin = turns(q * points, inner)
            rows[share * block + row] = np.concatenate([-sin, cos] if part else [cos, sin])
            cos, sin = turns((q + 1) * points, inner)
            rows[(shares + share) * block + row] = np.concatenate([-sin, -cos] if part else [cos, -sin])
    return rows


def square_table(inner):
    cos, sin = turns(np.arange(inner)[:, None] * np.arange(inner)[None, :], inner)
    return np.block([[cos, -sin], [sin, cos]])


def scaled(value, cos, sin):
    real, imag = value
    if abs(sin) < 1e-12:
        return (real, imag) if cos > 0 else (-real, -imag)
    if abs(cos) < 1e-12:
        return (-imag, real) if sin > 0 else (imag, -real)
    if abs(abs(cos) - abs(sin)) < 1e-12:
        size = abs(cos)
        a, b = (1.0 if cos > 0 else -1.0), (1.0 if sin > 0 else -1.0)
        first = (real if a > 0 else -real) + (-imag if b > 0 else imag)
        second = (real if b > 0 else -real) + (imag if a > 0 else -imag)
        return first * size, second * size
    return real * cos - imag * sin, real * sin + imag * cos


def unit(step, size, direction):
    angle = direction * 2.0 * math.pi * step / size
    return math.cos(angle), math.sin(angle)


def complex_fft(values, direction):
    size = len(values)
    if size == 1:
        return values
    even = complex_fft(values[0::2], direction)
    odd = complex_fft(values[1::2], direction)
    first, second = [], []
    for k in range(size // 2):
        real, imag = scaled(odd[k], *unit(k, size, direction))
        first.append((even[k][0] + real, even[k][1] + imag))
        second.append((even[k][0] - real, even[k][1] - imag))
    return first + second


def real_fft(values):
    size = len(values)
    if size == 2:
        return [(values[0] + values[1], None), (values[0] - values[1], None)]
    even = real_fft(values[0::2])
    odd = real_fft(values[1::2])
    quarter = size // 4
    out = [None] * (size // 2 + 1)
    out[0] = (even[0][0] + odd[0][0], None)
    out[size // 2] = (even[0][0] - odd[0][0], None)
    for k in range(1, quarter):
        real, imag = scaled(odd[k], *unit(k, size, -1.0))
        out[k] = (even[k][0] + real, even[k][1] + imag)
        out[size // 2 - k] = (even[k][0] - real, imag - even[k][1])
    out[quarter] = (even[quarter][0], -odd[quarter][0])
    return out


def real_sum(values):
    count = len(values) - 1
    size = 2 * count
    if size == 2:
        return [values[0][0] + values[1][0], values[0][0] - values[1][0]]
    half = count // 2
    even = [(values[0][0] + values[count][0], None)]
    odd = [(values[0][0] - values[count][0], None)]
    for s in range(1, half):
        near, far = values[s], values[count - s]
        even.append((near[0] + far[0], near[1] - far[1]))
        odd.append(scaled((near[0] - far[0], near[1] + far[1]), *unit(s, size, 1.0)))
    even.append((values[half][0], None))
    odd.append((-values[half][1], None))
    even_out, odd_out = real_sum(even), real_sum(odd)
    out = []
    for m in range(count):
        out += [even_out[m], odd_out[m]]
    return out


def three_products(left, right, dims):
    left_high, left_low = left
    right_high, right_low = right

    def one(a, b):
        return lax.dot_general(a, b, (dims, ((), ())), preferred_element_type=jnp.float32)

    return one(left_high, right_high) + one(left_low, right_high) + one(left_high, right_low)


def slot_order():
    return [0, radix // 2] + list(range(1, radix // 2))


def rows_forward(x_ref, high_ref, low_ref, cos_ref, sin_ref, out_ref, th_ref, tl_ref, *, shares, block):
    rows, length = x_ref.shape[2:]
    inner = length // radix
    order = slot_order()
    chunk = 2 * tile

    def vector_stage(step, carry):
        start = pl.multiple_of(step * chunk, chunk)
        for column in range(0, inner, lane):
            parts = [
                x_ref[0, 0, pl.ds(start, chunk), a * inner + column : a * inner + column + lane]
                for a in range(radix)
            ]
            spectrum = real_fft(parts)
            for slot, s in enumerate(order):
                real, imag = spectrum[s]
                if s:
                    cos = cos_ref[s : s + 1, column : column + lane]
                    sin = sin_ref[s : s + 1, column : column + lane]
                    if imag is None:
                        real, imag = real * cos, -(real * sin)
                    else:
                        real, imag = real * cos + imag * sin, imag * cos - real * sin
                else:
                    imag = jnp.zeros_like(real)
                where = pl.ds(pl.multiple_of(slot * rows + start, chunk), chunk)
                for offset, part in ((0, real), (inner, imag)):
                    high, low = split_parts(part)
                    th_ref[where, offset + column : offset + column + lane] = high
                    tl_ref[where, offset + column : offset + column + lane] = low
        return carry

    lax.fori_loop(0, rows // chunk, vector_stage, 0)
    nt = ((1,), (1,))
    single = shares * block
    slot = 0
    while slot < len(order):
        count = min(2, len(order) - slot)
        height = single if slot == 0 else 2 * single
        where = slice(slot * rows, (slot + count) * rows)
        result = three_products(
            (high_ref[:height], low_ref[:height]), (th_ref[where], tl_ref[where]), nt
        )
        for index in range(count):
            s = order[slot + index]
            columns = result[:, index * rows : (index + 1) * rows]
            for share in range(shares):
                out_ref[s * shares + share] = columns[share * block : (share + 1) * block]
                if slot:
                    out_ref[(radix - s) * shares + share] = columns[
                        single + share * block : single + (share + 1) * block
                    ]
        slot += count


def rows_back(in_ref, high_ref, low_ref, cos_ref, sin_ref, out_ref, g_ref, *, shares, block):
    rows, length = out_ref.shape[2:]
    inner = length // radix
    order = slot_order()
    depth = high_ref.shape[0]
    for slot, s in enumerate(order):
        blocks = [in_ref[s * shares + share] for share in range(shares)]
        if slot > 1:
            blocks += [in_ref[(radix - s) * shares + share] for share in range(shares)]
        used = len(blocks) * block
        wide = -(-used // lane) * lane
        if wide > used:
            blocks.append(jnp.zeros((wide - used, rows), jnp.float32))
        turned = jnp.transpose(jnp.concatenate(blocks, axis=0))
        keep = slice(0, wide)
        g_ref[slot * rows : (slot + 1) * rows] = three_products(
            split_parts(turned), (high_ref[keep], low_ref[keep]), ((1,), (0,))
        )
    chunk = tile

    def vector_stage(step, carry):
        start = pl.multiple_of(step * chunk, chunk)
        for column in range(0, inner, lane):
            values = [None] * len(order)
            for slot, s in enumerate(order):
                where = pl.ds(pl.multiple_of(slot * rows + start, chunk), chunk)
                real = g_ref[where, column : column + lane]
                if s:
                    imag = g_ref[where, inner + column : inner + column + lane]
                    cos = cos_ref[s : s + 1, column : column + lane]
                    sin = sin_ref[s : s + 1, column : column + lane]
                    if 2 * s == radix:
                        real, imag = real * cos - imag * sin, None
                    else:
                        real, imag = real * cos - imag * sin, real * sin + imag * cos
                else:
                    imag = None
                values[s] = (real, imag)
            for a, out in enumerate(real_sum(values)):
                out_ref[0, 0, pl.ds(start, chunk), a * inner + column : a * inner + column + lane] = out
        return carry

    lax.fori_loop(0, rows // chunk, vector_stage, 0)


def lines_middle(
    index_ref, wave_ref, in_ref, high_ref, low_ref, cos_ref, sin_ref, out_ref, th_ref, tl_ref, x_ref,
    *, components, shares, block, per_device, keep_x, length_x
):
    rows = in_ref.shape[2]
    inner = shares * rows
    length_y = radix * inner
    main = per_device // tile * tile
    chunk = 2 * tile
    padded = -(-(main + tile) // chunk) * chunk
    group = radix * padded
    half = tile // 2

    def read(c, source, start):
        real, imag = [], []
        for row in range(start, start + chunk, tile):
            if row < main:
                real.append(in_ref[source, pl.ds(c * block + row, tile), :])
                imag.append(in_ref[source, pl.ds(c * block + main + row, tile), :])
            elif row == main:
                last = in_ref[source, pl.ds(c * block + 2 * main, tile), :]
                real.append(last)
                imag.append(pltpu.roll(last, half, 0))
            else:
                real.append(jnp.zeros((tile, rows), jnp.float32))
                imag.append(jnp.zeros((tile, rows), jnp.float32))
        return jnp.concatenate(real, axis=0), jnp.concatenate(imag, axis=0)

    def write(c, target, start, real, imag):
        for position, row in enumerate(range(start, start + chunk, tile)):
            a = real[position * tile : (position + 1) * tile]
            b = imag[position * tile : (position + 1) * tile]
            if row < main:
                out_ref[target, pl.ds(c * block + row, tile), :] = a
                out_ref[target, pl.ds(c * block + main + row, tile), :] = b
            elif row == main:
                index = lax.broadcasted_iota(jnp.int32, (tile, rows), 0)
                out_ref[target, pl.ds(c * block + 2 * main, tile), :] = jnp.where(
                    index < half, a, pltpu.roll(b, half, 0)
                )

    def forward(c, carry):
        for start in range(0, padded, chunk):
            for share in range(shares):
                column = share * rows
                values = [read(c, a * shares + share, start) for a in range(radix)]
                for s, (real, imag) in enumerate(complex_fft(values, -1.0)):
                    if s:
                        cos = cos_ref[s : s + 1, column : column + rows]
                        sin = sin_ref[s : s + 1, column : column + rows]
                        real, imag = real * cos + imag * sin, imag * cos - real * sin
                    where = slice(s * padded + start, s * padded + start + chunk)
                    for offset, part in ((0, real), (inner, imag)):
                        high, low = split_parts(part)
                        th_ref[c, where, offset + column : offset + column + rows] = high
                        tl_ref[c, where, offset + column : offset + column + rows] = low
        return carry

    lax.fori_loop(0, components, forward, 0)

    def products(dims):
        def run(step, carry):
            c = step // 2
            where = pl.ds(pl.multiple_of((step % 2) * (group // 2), chunk), group // 2)
            x_ref[c, where, :] = three_products(
                (th_ref[c, where, :], tl_ref[c, where, :]), (high_ref[...], low_ref[...]), dims
            )
            return carry

        lax.fori_loop(0, 2 * components, run, 0)

    products(((1,), (0,)))

    share_of = index_ref[0] % shares
    offset_of = index_ref[0] // shares
    wave_z = wave_ref[0]
    scale = 1.0 / (length_x * length_y)

    def middle(s, carry):
        for start in range(0, padded, chunk):
            line = lax.broadcasted_iota(jnp.int32, (chunk, inner), 0) + start
            line_x = (share_of * per_device + line) * radix + offset_of
            index_y = lax.broadcasted_iota(jnp.int32, (chunk, inner), 1) * radix + s
            signed_y = jnp.where(index_y <= length_y // 2, index_y, index_y - length_y)
            kept = (line < per_device) & (line_x < keep_x) & (jnp.abs(signed_y) <= length_y // 3)
            weight = jnp.where(line_x == 0, scale, 2.0 * scale)
            factor = jnp.where(kept, weight, 0.0)
            wave_x = line_x.astype(jnp.float32)
            wave_y = signed_y.astype(jnp.float32)
            waves = (wave_x, wave_y, wave_z)
            inverse = factor / (wave_x * wave_x + wave_y * wave_y + wave_z * wave_z)
            where = pl.ds(pl.multiple_of(s * padded + start, chunk), chunk)
            for offset in (0, inner):
                columns = slice(offset, offset + inner)
                values = [x_ref[c, where, columns] for c in range(components)]
                divergence = (
                    wave_x * values[0] + wave_y * values[1] + wave_z * values[2]
                ) * inverse
                for c in range(components):
                    high, low = split_parts(factor * values[c] - waves[c] * divergence)
                    th_ref[c, where, columns] = high
                    tl_ref[c, where, columns] = low
        return carry

    lax.fori_loop(0, radix, middle, 0)
    products(((1,), (1,)))

    def backward(c, carry):
        for start in range(0, padded, chunk):
            for share in range(shares):
                column = share * rows
                values = []
                for s in range(radix):
                    where = slice(s * padded + start, s * padded + start + chunk)
                    real = x_ref[c, where, column : column + rows]
                    imag = x_ref[c, where, inner + column : inner + column + rows]
                    if s:
                        cos = cos_ref[s : s + 1, column : column + rows]
                        sin = sin_ref[s : s + 1, column : column + rows]
                        real, imag = real * cos - imag * sin, real * sin + imag * cos
                    values.append((real, imag))
                for a, (real, imag) in enumerate(complex_fft(values, 1.0)):
                    write(c, a * shares + share, start, real, imag)
        return carry

    lax.fori_loop(0, components, backward, 0)


def whole(shape):
    return pl.BlockSpec(shape, lambda *_: (0,) * len(shape))


def local_fast(velocity, plane_wavenumber):
    components, _, rows, length_x = velocity.shape
    devices = lax.axis_size("wide") * lax.axis_size("narrow")
    keep_x = length_x // 3 + 1
    inner = length_x // radix
    shares = devices // radix
    per_device = -(-keep_x // (radix * shares))
    main = per_device // tile * tile
    block = 2 * main + tile
    padded = -(-(main + tile) // (2 * tile)) * 2 * tile
    table = row_table(inner, per_device, shares, block)
    table = np.pad(table, ((0, -len(table) % lane), (0, 0)))
    row_high, row_low = (jnp.asarray(t) for t in split_table(table))
    line_inner = shares * rows
    line_high, line_low = (jnp.asarray(t) for t in split_table(square_table(line_inner)))
    row_cos, row_sin = (jnp.asarray(t, jnp.float32) for t in twist_table(inner))
    line_cos, line_sin = (jnp.asarray(t, jnp.float32) for t in twist_table(line_inner))
    limits = pltpu.CompilerParams(vmem_limit_bytes=56 * 1024 * 1024)
    row_tables = (row_high, row_low, row_cos, row_sin)
    row_specs = [whole(t.shape) for t in row_tables]
    slots = radix // 2 + 1
    field_spec = pl.BlockSpec((1, 1, rows, length_x), lambda c: (c, 0, 0, 0))
    line_spec = pl.BlockSpec((devices, block, rows), lambda c: (0, c, 0))
    line_shape = jax.ShapeDtypeStruct((devices, components * block, rows), jnp.float32)
    spectrum = pl.pallas_call(
        lambda *refs: rows_forward(*refs, shares=shares, block=block),
        grid=(components,),
        in_specs=[field_spec] + row_specs,
        out_specs=line_spec,
        out_shape=line_shape,
        scratch_shapes=[pltpu.VMEM((slots * rows, 2 * inner), jnp.bfloat16)] * 2,
        compiler_params=limits,
        name="rows_forward",
    )(velocity, *row_tables)
    lines = lax.all_to_all(spectrum, axes, split_axis=0, concat_axis=0, tiled=True)
    index = lax.axis_index(axes).astype(jnp.int32).reshape(1)
    line_tables = (line_high, line_low, line_cos, line_sin)
    scalar = pl.BlockSpec(memory_space=pltpu.SMEM)
    solved = pl.pallas_call(
        lambda *refs: lines_middle(
            *refs, components=components, shares=shares, block=block, per_device=per_device,
            keep_x=keep_x, length_x=length_x,
        ),
        grid=(1,),
        in_specs=[scalar, scalar, whole(line_shape.shape)] + [whole(t.shape) for t in line_tables],
        out_specs=whole(line_shape.shape),
        out_shape=line_shape,
        scratch_shapes=[pltpu.VMEM((components, radix * padded, 2 * line_inner), jnp.bfloat16)] * 2
        + [pltpu.VMEM((components, radix * padded, 2 * line_inner), jnp.float32)],
        compiler_params=limits,
        name="lines_middle",
    )(index, plane_wavenumber, lines, *line_tables)
    returned = lax.all_to_all(solved, axes, split_axis=0, concat_axis=0, tiled=True)
    return pl.pallas_call(
        lambda *refs: rows_back(*refs, shares=shares, block=block),
        grid=(components,),
        in_specs=[line_spec] + row_specs,
        out_specs=field_spec,
        out_shape=jax.ShapeDtypeStruct(velocity.shape, jnp.float32),
        scratch_shapes=[pltpu.VMEM((slots * rows, 2 * inner), jnp.float32)],
        compiler_params=limits,
        name="rows_back",
    )(returned, *row_tables)


def local(velocity, plane_wavenumber):
    components, planes, rows, length_x = velocity.shape
    devices = lax.axis_size("wide") * lax.axis_size("narrow")
    keep_x = length_x // 3 + 1
    fits = (
        components == 3
        and planes == 1
        and rows == lane
        and length_x % (radix * lane) == 0
        and devices % radix == 0
        and -(-keep_x // devices) == -(-(-(-keep_x // radix)) // (devices // radix))
        and -(-keep_x // devices) % tile <= tile // 2
        and (rows * devices) // 3 < rows * devices // 2
    )
    if fits:
        return local_fast(velocity, plane_wavenumber)
    return local_generic(velocity, plane_wavenumber)


def solution(mesh):
    placed = (P(None, None, ("wide", "narrow"), None), P())
    return jax.shard_map(
        local,
        mesh=mesh,
        in_specs=placed,
        out_specs=P(None, None, ("wide", "narrow"), None),
        check_vma=False,
    )
```

```python
import functools
import math

import jax
import jax.numpy as jnp
import numpy as np
from jax import lax
from jax.experimental import pallas as pl
from jax.experimental.pallas import tpu as pltpu
from jax.sharding import PartitionSpec as P


radix_split = 64
highest = lax.Precision.HIGHEST


def angle_tables(row_size, col_size, period, direction):
    product = jnp.arange(row_size)[:, None] * jnp.arange(col_size)[None, :] % period
    angles = direction * 2.0 * math.pi * product.astype(jnp.float32) / period
    return (jnp.cos(angles), jnp.sin(angles))


def complex_product(pattern, left_real, left_imag, table_real, table_imag):
    out_real = jnp.einsum(pattern, left_real, table_real, precision=highest) - jnp.einsum(
        pattern, left_imag, table_imag, precision=highest
    )
    out_imag = jnp.einsum(pattern, left_real, table_imag, precision=highest) + jnp.einsum(
        pattern, left_imag, table_real, precision=highest
    )
    return (out_real, out_imag)


def transform(real_part, imag_part, direction):
    length = real_part.shape[-1]
    inner_size = length // radix_split
    leading = real_part.shape[:-1]
    grid_real = real_part.reshape(leading + (radix_split, inner_size))
    grid_imag = imag_part.reshape(leading + (radix_split, inner_size))
    outer_cos, outer_sin = angle_tables(radix_split, radix_split, radix_split, direction)
    section_real, section_imag = complex_product(
        "...ab,ak->...kb", grid_real, grid_imag, outer_cos, outer_sin
    )
    twist_cos, twist_sin = angle_tables(radix_split, inner_size, length, direction)
    turned_real = section_real * twist_cos - section_imag * twist_sin
    turned_imag = section_real * twist_sin + section_imag * twist_cos
    inner_cos, inner_sin = angle_tables(inner_size, inner_size, inner_size, direction)
    final_real, final_imag = complex_product(
        "...kb,bm->...mk", turned_real, turned_imag, inner_cos, inner_sin
    )
    return (final_real.reshape(leading + (length,)), final_imag.reshape(leading + (length,)))


def project(lines, wave_x, wave_z, kept_line):
    groups, per_device, length_y = lines.shape
    shaped = lines.reshape(3, 2, groups // 6, per_device, length_y)
    spec_real, spec_imag = transform(shaped[:, 0], shaped[:, 1], -1.0)
    index_y = jnp.arange(length_y)
    signed_y = jnp.where(index_y <= length_y // 2, index_y, index_y - length_y)
    kept_y = jnp.abs(signed_y) <= length_y // 3
    retained = (kept_line & kept_y[None, None, :]).astype(jnp.float32)
    wave_y = signed_y.astype(jnp.float32)[None, None, :]
    wave_square = wave_x * wave_x + wave_y * wave_y + wave_z * wave_z
    waves = (wave_x, wave_y, wave_z)
    div_real = wave_x * spec_real[0] + wave_y * spec_real[1] + wave_z * spec_real[2]
    div_imag = wave_x * spec_imag[0] + wave_y * spec_imag[1] + wave_z * spec_imag[2]
    proj_real = jnp.stack(
        [
            (spec_real[component] - waves[component] * div_real / wave_square) * retained
            for component in range(3)
        ]
    )
    proj_imag = jnp.stack(
        [
            (spec_imag[component] - waves[component] * div_imag / wave_square) * retained
            for component in range(3)
        ]
    )
    back_real, back_imag = transform(proj_real, proj_imag, 1.0)
    return jnp.stack([back_real / length_y, back_imag / length_y], axis=1).reshape(
        groups, per_device, length_y
    )


def first_send(spectrum, first_size):
    groups, rows, span = spectrum.shape
    return (
        spectrum.reshape(groups, rows, first_size, span // first_size)
        .transpose(2, 0, 1, 3)
        .reshape(first_size, 1, -1)
    )


def second_send(received, first_size, second_size, groups, rows, per_device):
    shaped = received.reshape(first_size, groups, rows, second_size, per_device)
    return shaped.transpose(3, 1, 4, 0, 2).reshape(second_size, 1, -1)


def arrange_lines(received, first_size, second_size, groups, rows, per_device):
    shaped = received.reshape(second_size, groups, per_device, first_size, rows)
    ordered = shaped.transpose(1, 2, 0, 3, 4)
    return ordered.reshape(groups, per_device, -1)


def first_return(solved, first_size, second_size, rows):
    groups, per_device, _ = solved.shape
    shaped = solved.reshape(groups, per_device, second_size, first_size, rows).transpose(
        2, 0, 1, 3, 4
    )
    return shaped.reshape(second_size, 1, -1)


def second_return(received, first_size, second_size, groups, rows, per_device):
    shaped = received.reshape(second_size, groups, per_device, first_size, rows)
    return shaped.transpose(3, 1, 4, 0, 2).reshape(first_size, 1, -1)


def arrange_rows(received, first_size, groups, rows):
    shaped = received.reshape(first_size, groups, rows, -1)
    return shaped.transpose(1, 2, 0, 3).reshape(groups, rows, -1)


def local_generic(velocity, plane_wavenumber):
    components, plane_count, row_count, x_length = velocity.shape
    wide_size = lax.axis_size("wide")
    narrow_size = lax.axis_size("narrow")
    device_count = wide_size * narrow_size
    keep_x = x_length // 3 + 1
    spec_real, spec_imag = transform(velocity, jnp.zeros_like(velocity), -1.0)
    spec_real = spec_real[..., :keep_x]
    spec_imag = spec_imag[..., :keep_x]
    per_device = (keep_x + device_count - 1) // device_count
    line_span = per_device * device_count
    gap = ((0, 0), (0, 0), (0, 0), (0, 0), (0, line_span - keep_x))
    stacked = jnp.stack([spec_real, spec_imag], axis=1)
    spectrum = jnp.pad(stacked, gap).reshape(components * 2 * plane_count, row_count, line_span)
    groups = spectrum.shape[0]
    halfway = lax.all_to_all(
        first_send(spectrum, narrow_size), "narrow", split_axis=0, concat_axis=1, tiled=True
    )
    outgoing = second_send(halfway, narrow_size, wide_size, groups, row_count, per_device)
    arrived = lax.all_to_all(outgoing, "wide", split_axis=0, concat_axis=1, tiled=True)
    lines = arrange_lines(arrived, narrow_size, wide_size, groups, row_count, per_device)
    line_start = (
        lax.axis_index("narrow") * (per_device * wide_size) + lax.axis_index("wide") * per_device
    )
    indices = line_start + jnp.arange(per_device)
    wave_x = indices.astype(jnp.float32)[None, :, None]
    wave_z = plane_wavenumber[:, None, None]
    kept_line = (indices < keep_x)[None, :, None]
    solved = project(lines, wave_x, wave_z, kept_line)
    halfway = lax.all_to_all(
        first_return(solved, narrow_size, wide_size, row_count),
        "wide",
        split_axis=0,
        concat_axis=1,
        tiled=True,
    )
    outgoing = second_return(halfway, narrow_size, wide_size, groups, row_count, per_device)
    arrived = lax.all_to_all(outgoing, "narrow", split_axis=0, concat_axis=1, tiled=True)
    returned = arrange_rows(arrived, narrow_size, groups, row_count)
    columns = returned.reshape(components, 2, plane_count, row_count, line_span)[..., :keep_x]
    weights = jnp.where(jnp.arange(keep_x) == 0, 1.0, 2.0).astype(jnp.float32)
    widen = ((0, 0), (0, 0), (0, 0), (0, x_length - keep_x))
    back_real = jnp.pad(columns[:, 0] * weights, widen)
    back_imag = jnp.pad(columns[:, 1] * weights, widen)
    out_real, _ = transform(back_real, back_imag, 1.0)
    return out_real / x_length


radix = 16
lane = 128
tile = 8
axes = ("wide", "narrow")


def split_parts(values):
    high = values.astype(jnp.bfloat16)
    low = (values - high.astype(jnp.float32)).astype(jnp.bfloat16)
    return high, low


def split_table(values):
    values = values.astype(np.float32)
    high = values.astype(jnp.bfloat16)
    low = (values - high.astype(np.float32)).astype(jnp.bfloat16)
    return high, low


def turns(product, period):
    angle = 2.0 * np.pi * (np.asarray(product) % period) / period
    return np.cos(angle), np.sin(angle)


def twist_table(inner):
    return turns(np.arange(radix)[:, None] * np.arange(inner)[None, :], radix * inner)


def line_chunks(per_device):
    first = per_device // (4 * tile) * (2 * tile)
    last = per_device - first
    main = last // tile * tile
    return ((0, first, first, 2 * first), (first, last, main, 2 * main + tile))


def line_slots(per_device):
    half = tile // 2
    base = 0
    slots = []
    for start, lines, main, height in line_chunks(per_device):
        slots += [(base + line, start + line, 0) for line in range(main)]
        slots += [(base + main + line, start + line, 1) for line in range(main)]
        for extra in range(lines - main):
            slots.append((base + 2 * main + extra, start + main + extra, 0))
            slots.append((base + 2 * main + half + extra, start + main + extra, 1))
        base += height
    return slots


def row_table(inner, per_device, shares, block):
    rows = np.zeros((2 * shares * block, 2 * inner))
    points = np.arange(inner)
    for share in range(shares):
        for row, line, part in line_slots(per_device):
            q = share * per_device + line
            cos, sin = turns(q * points, inner)
            rows[share * block + row] = np.concatenate([-sin, cos] if part else [cos, sin])
            cos, sin = turns((q + 1) * points, inner)
            rows[(shares + share) * block + row] = np.concatenate([-sin, -cos] if part else [cos, -sin])
    return rows


def square_table(inner):
    cos, sin = turns(np.arange(inner)[:, None] * np.arange(inner)[None, :], inner)
    return np.block([[cos, -sin], [sin, cos]])


def scaled(value, cos, sin):
    real, imag = value
    if abs(sin) < 1e-12:
        return (real, imag) if cos > 0 else (-real, -imag)
    if abs(cos) < 1e-12:
        return (-imag, real) if sin > 0 else (imag, -real)
    if abs(abs(cos) - abs(sin)) < 1e-12:
        size = abs(cos)
        a, b = (1.0 if cos > 0 else -1.0), (1.0 if sin > 0 else -1.0)
        first = (real if a > 0 else -real) + (-imag if b > 0 else imag)
        second = (real if b > 0 else -real) + (imag if a > 0 else -imag)
        return first * size, second * size
    return real * cos - imag * sin, real * sin + imag * cos


def unit(step, size, direction):
    angle = direction * 2.0 * math.pi * step / size
    return math.cos(angle), math.sin(angle)


def complex_fft(values, direction):
    size = len(values)
    if size == 1:
        return values
    even = complex_fft(values[0::2], direction)
    odd = complex_fft(values[1::2], direction)
    first, second = [], []
    for k in range(size // 2):
        real, imag = scaled(odd[k], *unit(k, size, direction))
        first.append((even[k][0] + real, even[k][1] + imag))
        second.append((even[k][0] - real, even[k][1] - imag))
    return first + second


def real_fft(values):
    size = len(values)
    if size == 2:
        return [(values[0] + values[1], None), (values[0] - values[1], None)]
    even = real_fft(values[0::2])
    odd = real_fft(values[1::2])
    quarter = size // 4
    out = [None] * (size // 2 + 1)
    out[0] = (even[0][0] + odd[0][0], None)
    out[size // 2] = (even[0][0] - odd[0][0], None)
    for k in range(1, quarter):
        real, imag = scaled(odd[k], *unit(k, size, -1.0))
        out[k] = (even[k][0] + real, even[k][1] + imag)
        out[size // 2 - k] = (even[k][0] - real, imag - even[k][1])
    out[quarter] = (even[quarter][0], -odd[quarter][0])
    return out


def real_sum(values):
    count = len(values) - 1
    size = 2 * count
    if size == 2:
        return [values[0][0] + values[1][0], values[0][0] - values[1][0]]
    half = count // 2
    even = [(values[0][0] + values[count][0], None)]
    odd = [(values[0][0] - values[count][0], None)]
    for s in range(1, half):
        near, far = values[s], values[count - s]
        even.append((near[0] + far[0], near[1] - far[1]))
        odd.append(scaled((near[0] - far[0], near[1] + far[1]), *unit(s, size, 1.0)))
    even.append((values[half][0], None))
    odd.append((-values[half][1], None))
    even_out, odd_out = real_sum(even), real_sum(odd)
    out = []
    for m in range(count):
        out += [even_out[m], odd_out[m]]
    return out


def three_products(left, right, dims):
    left_high, left_low = left
    right_high, right_low = right

    def one(a, b):
        return lax.dot_general(a, b, (dims, ((), ())), preferred_element_type=jnp.float32)

    return one(left_high, right_high) + one(left_low, right_high) + one(left_high, right_low)


def slot_order():
    return [0, radix // 2] + list(range(1, radix // 2))


def rows_forward(
    index_ref, x_ref, high_ref, low_ref, cos_ref, sin_ref, near_ref, *refs, shares, block
):
    far_refs = refs[:-3]
    th_ref, tl_ref, box_ref = refs[-3:]
    split = near_ref.shape[1]
    rows, length = x_ref.shape[2:]
    inner = length // radix
    order = slot_order()
    chunk = 2 * tile

    def vector_stage(step, carry):
        start = pl.multiple_of(step * chunk, chunk)
        for column in range(0, inner, lane):
            parts = [
                x_ref[0, 0, pl.ds(start, chunk), a * inner + column : a * inner + column + lane]
                for a in range(radix)
            ]
            spectrum = real_fft(parts)
            for slot, s in enumerate(order):
                real, imag = spectrum[s]
                if s:
                    cos = cos_ref[s : s + 1, column : column + lane]
                    sin = sin_ref[s : s + 1, column : column + lane]
                    if imag is None:
                        real, imag = real * cos, -(real * sin)
                    else:
                        real, imag = real * cos + imag * sin, imag * cos - real * sin
                else:
                    imag = jnp.zeros_like(real)
                where = pl.ds(pl.multiple_of(slot * rows + start, chunk), chunk)
                for offset, part in ((0, real), (inner, imag)):
                    high, low = split_parts(part)
                    th_ref[where, offset + column : offset + column + lane] = high
                    tl_ref[where, offset + column : offset + column + lane] = low
        return carry

    lax.fori_loop(0, rows // chunk, vector_stage, 0)
    nt = ((1,), (1,))
    single = shares * block
    slot = 0
    while slot < len(order):
        count = min(2, len(order) - slot)
        height = single if slot == 0 else 2 * single
        where = slice(slot * rows, (slot + count) * rows)
        result = three_products(
            (high_ref[:height], low_ref[:height]), (th_ref[where], tl_ref[where]), nt
        )
        for index in range(count):
            s = order[slot + index]
            columns = result[:, index * rows : (index + 1) * rows]
            for share in range(shares):
                targets = [(s, share)] + ([(radix - s, shares + share)] if slot else [])
                for residue, position in targets:
                    piece = columns[position * block : (position + 1) * block]
                    near_ref[residue * shares + share] = piece[:split]
                    box_ref[residue * shares + share] = piece[split:]
        slot += count
    height = block - split
    where = pl.ds(pl.program_id(0) * height, height)
    for k, far_ref in enumerate(far_refs):
        far_ref[where, :] = box_ref[index_ref[0] ^ k]


def rows_back(index_ref, near_ref, high_ref, low_ref, cos_ref, sin_ref, *refs, shares, block):
    out_ref, g_ref, far_ref = refs[-3:]
    devices, height = far_ref.shape[:2]
    place = pl.ds(pl.program_id(0) * height, height)
    for k in range(devices):
        far_ref[index_ref[0] ^ k] = refs[k][place, :]
    rows, length = out_ref.shape[2:]
    inner = length // radix
    order = slot_order()
    for slot, s in enumerate(order):
        blocks = []
        for residue in [s] if slot < 2 else [s, radix - s]:
            for share in range(shares):
                blocks += [near_ref[residue * shares + share], far_ref[residue * shares + share]]
        used = len(blocks) // 2 * block
        wide = -(-used // lane) * lane
        if wide > used:
            blocks.append(jnp.zeros((wide - used, rows), jnp.float32))
        turned = jnp.transpose(jnp.concatenate(blocks, axis=0))
        keep = slice(0, wide)
        g_ref[slot * rows : (slot + 1) * rows] = three_products(
            split_parts(turned), (high_ref[keep], low_ref[keep]), ((1,), (0,))
        )
    chunk = tile

    def vector_stage(step, carry):
        start = pl.multiple_of(step * chunk, chunk)
        for column in range(0, inner, lane):
            values = [None] * len(order)
            for slot, s in enumerate(order):
                where = pl.ds(pl.multiple_of(slot * rows + start, chunk), chunk)
                real = g_ref[where, column : column + lane]
                if s:
                    imag = g_ref[where, inner + column : inner + column + lane]
                    cos = cos_ref[s : s + 1, column : column + lane]
                    sin = sin_ref[s : s + 1, column : column + lane]
                    if 2 * s == radix:
                        real, imag = real * cos - imag * sin, None
                    else:
                        real, imag = real * cos - imag * sin, real * sin + imag * cos
                else:
                    imag = None
                values[s] = (real, imag)
            for a, out in enumerate(real_sum(values)):
                out_ref[0, 0, pl.ds(start, chunk), a * inner + column : a * inner + column + lane] = out
        return carry

    lax.fori_loop(0, rows // chunk, vector_stage, 0)


def lines_middle(
    index_ref, wave_ref, *refs, counts, targets, shares, chunk_shape, per_device, keep_x, length_x
):
    in_refs = refs[: len(counts)]
    high_ref, low_ref, cos_ref, sin_ref = refs[len(counts) : len(counts) + 4]
    th_ref, tl_ref, x_ref = refs[-3:]
    out_refs = refs[-3 - len(targets) : -3]
    first, lines, main, block = chunk_shape
    components = sum(counts)
    rows = in_refs[0].shape[2]
    inner = shares * rows
    length_y = radix * inner
    chunk = 2 * tile
    padded = -(-lines // chunk) * chunk
    group = radix * padded
    half = tile // 2

    def read(in_ref, c, source, start):
        real, imag = [], []
        for row in range(start, start + chunk, tile):
            if row < main:
                real.append(in_ref[source, pl.ds(c * block + row, tile), :])
                imag.append(in_ref[source, pl.ds(c * block + main + row, tile), :])
            elif row == main:
                last = in_ref[source, pl.ds(c * block + 2 * main, tile), :]
                real.append(last)
                imag.append(pltpu.roll(last, half, 0))
            else:
                real.append(jnp.zeros((tile, rows), jnp.float32))
                imag.append(jnp.zeros((tile, rows), jnp.float32))
        return jnp.concatenate(real, axis=0), jnp.concatenate(imag, axis=0)

    def write(out_ref, c, target, start, real, imag):
        for position, row in enumerate(range(start, start + chunk, tile)):
            a = real[position * tile : (position + 1) * tile]
            b = imag[position * tile : (position + 1) * tile]
            if row < main:
                out_ref[target, pl.ds(c * block + row, tile), :] = a
                out_ref[target, pl.ds(c * block + main + row, tile), :] = b
            elif row == main:
                index = lax.broadcasted_iota(jnp.int32, (tile, rows), 0)
                out_ref[target, pl.ds(c * block + 2 * main, tile), :] = jnp.where(
                    index < half, a, pltpu.roll(b, half, 0)
                )

    def forward(in_ref, base, position, carry):
        c = base + position
        for start in range(0, padded, chunk):
            for share in range(shares):
                column = share * rows
                values = [
                    read(in_ref, position, a * shares + share, start) for a in range(radix)
                ]
                for s, (real, imag) in enumerate(complex_fft(values, -1.0)):
                    if s:
                        cos = cos_ref[s : s + 1, column : column + rows]
                        sin = sin_ref[s : s + 1, column : column + rows]
                        real, imag = real * cos + imag * sin, imag * cos - real * sin
                    where = slice(s * padded + start, s * padded + start + chunk)
                    for offset, part in ((0, real), (inner, imag)):
                        high, low = split_parts(part)
                        th_ref[c, where, offset + column : offset + column + rows] = high
                        tl_ref[c, where, offset + column : offset + column + rows] = low
        return carry

    base = 0
    for in_ref, count in zip(in_refs, counts):
        lax.fori_loop(0, count, functools.partial(forward, in_ref, base), 0)
        base += count

    def products(dims):
        def run(step, carry):
            c = step // 2
            where = pl.ds(pl.multiple_of((step % 2) * (group // 2), chunk), group // 2)
            x_ref[c, where, :] = three_products(
                (th_ref[c, where, :], tl_ref[c, where, :]), (high_ref[...], low_ref[...]), dims
            )
            return carry

        lax.fori_loop(0, 2 * components, run, 0)

    products(((1,), (0,)))

    share_of = index_ref[0] % shares
    offset_of = index_ref[0] // shares
    wave_z = wave_ref[0]
    scale = 1.0 / (length_x * length_y)

    def middle(s, carry):
        for start in range(0, padded, chunk):
            line = lax.broadcasted_iota(jnp.int32, (chunk, inner), 0) + start
            line_x = (share_of * per_device + first + line) * radix + offset_of
            index_y = lax.broadcasted_iota(jnp.int32, (chunk, inner), 1) * radix + s
            signed_y = jnp.where(index_y <= length_y // 2, index_y, index_y - length_y)
            kept = (line < lines) & (line_x < keep_x) & (jnp.abs(signed_y) <= length_y // 3)
            weight = jnp.where(line_x == 0, scale, 2.0 * scale)
            factor = jnp.where(kept, weight, 0.0)
            wave_x = line_x.astype(jnp.float32)
            wave_y = signed_y.astype(jnp.float32)
            waves = (wave_x, wave_y, wave_z)
            inverse = factor / (wave_x * wave_x + wave_y * wave_y + wave_z * wave_z)
            where = pl.ds(pl.multiple_of(s * padded + start, chunk), chunk)
            for offset in (0, inner):
                columns = slice(offset, offset + inner)
                values = [x_ref[c, where, columns] for c in range(components)]
                divergence = (
                    wave_x * values[0] + wave_y * values[1] + wave_z * values[2]
                ) * inverse
                for c in range(components):
                    high, low = split_parts(factor * values[c] - waves[c] * divergence)
                    th_ref[c, where, columns] = high
                    tl_ref[c, where, columns] = low
        return carry

    lax.fori_loop(0, radix, middle, 0)
    products(((1,), (1,)))

    def backward(out_ref, base, position, carry):
        c = base + position
        for start in range(0, padded, chunk):
            for share in range(shares):
                column = share * rows
                values = []
                for s in range(radix):
                    where = slice(s * padded + start, s * padded + start + chunk)
                    real = x_ref[c, where, column : column + rows]
                    imag = x_ref[c, where, inner + column : inner + column + rows]
                    if s:
                        cos = cos_ref[s : s + 1, column : column + rows]
                        sin = sin_ref[s : s + 1, column : column + rows]
                        real, imag = real * cos - imag * sin, real * sin + imag * cos
                    values.append((real, imag))
                for a, (real, imag) in enumerate(complex_fft(values, 1.0)):
                    write(out_ref, position, a * shares + share, start, real, imag)
        return carry

    base = 0
    for out_ref, count in zip(out_refs, targets):
        lax.fori_loop(0, count, functools.partial(backward, out_ref, base), 0)
        base += count


def whole(shape):
    return pl.BlockSpec(shape, lambda *_: (0,) * len(shape))


def token_of(in_ref, out_ref):
    out_ref[...] = in_ref[0]


def exchange(values):
    return lax.all_to_all(values, axes, split_axis=0, concat_axis=0, tiled=True)


def swap(blocks):
    count = len(blocks)
    moved = list(blocks)
    for k in range(1, count):
        moved[k] = lax.ppermute(blocks[k], axes, [(source, source ^ k) for source in range(count)])
    return moved


def local_fast(velocity, plane_wavenumber):
    components, _, rows, length_x = velocity.shape
    devices = lax.axis_size("wide") * lax.axis_size("narrow")
    keep_x = length_x // 3 + 1
    inner = length_x // radix
    shares = devices // radix
    per_device = -(-keep_x // (radix * shares))
    near, far = line_chunks(per_device)
    block = near[3] + far[3]
    table = row_table(inner, per_device, shares, block)
    table = np.pad(table, ((0, -len(table) % lane), (0, 0)))
    line_inner = shares * rows
    row_tables = [jnp.asarray(t) for t in split_table(table)]
    row_tables += [jnp.asarray(t, jnp.float32) for t in twist_table(inner)]
    line_tables = [jnp.asarray(t) for t in split_table(square_table(line_inner))]
    line_tables += [jnp.asarray(t, jnp.float32) for t in twist_table(line_inner)]
    limits = pltpu.CompilerParams(vmem_limit_bytes=56 * 1024 * 1024)
    slots = radix // 2 + 1
    anywhere = pl.BlockSpec(memory_space=pl.ANY)
    scalar = pl.BlockSpec(memory_space=pltpu.SMEM)
    index = lax.axis_index(axes).astype(jnp.int32).reshape(1)

    def shape(count, height):
        return jax.ShapeDtypeStruct((devices, count * height, rows), jnp.float32)

    def single(count):
        return jax.ShapeDtypeStruct((count * far[3], rows), jnp.float32)

    def box(count):
        return pltpu.VMEM((devices, count * far[3], rows), jnp.float32)

    def component(height):
        return pl.BlockSpec((devices, height, rows), lambda c: (0, c, 0))

    field = pl.BlockSpec((1, 1, rows, length_x), lambda c: (c, 0, 0, 0))

    near_lines, *far_lines = pl.pallas_call(
        functools.partial(rows_forward, shares=shares, block=block),
        grid=(components,),
        in_specs=[scalar, field] + [whole(t.shape) for t in row_tables],
        out_specs=[component(near[3])] + [whole(single(components).shape)] * devices,
        out_shape=[shape(components, near[3])] + [single(components)] * devices,
        scratch_shapes=[pltpu.VMEM((slots * rows, 2 * inner), jnp.bfloat16)] * 2 + [box(1)],
        compiler_params=limits,
        name="rows_forward",
    )(index, velocity, *row_tables)

    def middle(sources, targets, chunk_shape):
        spread = len(sources) > 1
        height = chunk_shape[3]
        padded = -(-chunk_shape[1] // (2 * tile)) * 2 * tile
        group = (components, radix * padded, 2 * line_inner)
        outs = [shape(count, height) for count in targets]
        if spread:
            outs = outs[:-1] + [single(targets[-1])] * devices
        place = 2 + len(sources) + len(line_tables)

        def body(*refs):
            index_ref, wave_ref = refs[:2]
            from_refs, tables = refs[2 : 2 + len(sources)], refs[2 + len(sources) : place]
            to_refs, scratch = refs[place : place + len(outs)], refs[place + len(outs) :]
            spread_refs = to_refs[-devices:]
            if spread:
                in_box, out_box, *scratch = scratch
                for k, ref in enumerate(from_refs):
                    in_box[index_ref[0] ^ k] = ref[...]
                from_refs, to_refs = [in_box], to_refs[:-devices] + (out_box,)
            lines_middle(
                index_ref, wave_ref, *from_refs, *tables, *to_refs, *scratch, counts=(components,),
                targets=targets, shares=shares, chunk_shape=chunk_shape, per_device=per_device,
                keep_x=keep_x, length_x=length_x,
            )
            if spread:
                for k, ref in enumerate(spread_refs):
                    ref[...] = out_box[index_ref[0] ^ k]

        return pl.pallas_call(
            body,
            grid=(1,),
            in_specs=[scalar, scalar]
            + [whole(t.shape) for t in sources]
            + [whole(t.shape) for t in line_tables],
            out_specs=[whole(t.shape) for t in outs],
            out_shape=outs,
            scratch_shapes=([box(components), box(targets[-1])] if spread else [])
            + [pltpu.VMEM(group, jnp.bfloat16)] * 2
            + [pltpu.VMEM(group, jnp.float32)],
            compiler_params=limits,
        )(index, plane_wavenumber, *sources, *line_tables)

    def back(near_lines, far_lines, token):
        return pl.pallas_call(
            functools.partial(rows_back, shares=shares, block=block),
            grid=(components,),
            in_specs=[scalar, component(near[3])]
            + [whole(t.shape) for t in row_tables]
            + [whole(single(components).shape)] * devices
            + [anywhere],
            out_specs=field,
            out_shape=jax.ShapeDtypeStruct(velocity.shape, jnp.float32),
            scratch_shapes=[pltpu.VMEM((slots * rows, 2 * inner), jnp.float32), box(1)],
            compiler_params=limits,
            name="rows_back",
        )(index, near_lines, *row_tables, *far_lines, token)

    near_lines = exchange(near_lines)
    far_lines = swap(far_lines)
    (near_lines,) = middle([near_lines], (components,), near)
    near_lines = exchange(near_lines)
    far_lines = middle(far_lines, (components,), far)
    far_lines = swap(far_lines)
    token = pl.pallas_call(
        token_of,
        grid=(1,),
        in_specs=[pl.BlockSpec((1, tile, lane), lambda _: (0, 0, 0))],
        out_specs=whole((tile, lane)),
        out_shape=jax.ShapeDtypeStruct((tile, lane), jnp.float32),
        name="near_token",
    )(near_lines)
    return back(near_lines, far_lines, token)


def local(velocity, plane_wavenumber):
    components, planes, rows, length_x = velocity.shape
    devices = lax.axis_size("wide") * lax.axis_size("narrow")
    keep_x = length_x // 3 + 1
    fits = (
        components == 3
        and planes == 1
        and rows == lane
        and length_x % (radix * lane) == 0
        and devices % radix == 0
        and devices & (devices - 1) == 0
        and -(-keep_x // devices) == -(-(-(-keep_x // radix)) // (devices // radix))
        and -(-keep_x // devices) % tile <= tile // 2
        and (rows * devices) // 3 < rows * devices // 2
    )
    if fits:
        return local_fast(velocity, plane_wavenumber)
    return local_generic(velocity, plane_wavenumber)


def solution(mesh):
    placed = (P(None, None, ("wide", "narrow"), None), P())

    return jax.shard_map(
        local,
        mesh=mesh,
        in_specs=placed,
        out_specs=P(None, None, ("wide", "narrow"), None),
        check_vma=False,
    )
```

```python
import functools
import math

import jax
import jax.numpy as jnp
import numpy as np
from jax import lax
from jax.experimental import pallas as pl
from jax.experimental.pallas import tpu as pltpu
from jax.sharding import PartitionSpec as P


radix_split = 64
highest = lax.Precision.HIGHEST


def angle_tables(row_size, col_size, period, direction):
    product = jnp.arange(row_size)[:, None] * jnp.arange(col_size)[None, :] % period
    angles = direction * 2.0 * math.pi * product.astype(jnp.float32) / period
    return (jnp.cos(angles), jnp.sin(angles))


def complex_product(pattern, left_real, left_imag, table_real, table_imag):
    out_real = jnp.einsum(pattern, left_real, table_real, precision=highest) - jnp.einsum(
        pattern, left_imag, table_imag, precision=highest
    )
    out_imag = jnp.einsum(pattern, left_real, table_imag, precision=highest) + jnp.einsum(
        pattern, left_imag, table_real, precision=highest
    )
    return (out_real, out_imag)


def transform(real_part, imag_part, direction):
    length = real_part.shape[-1]
    inner_size = length // radix_split
    leading = real_part.shape[:-1]
    grid_real = real_part.reshape(leading + (radix_split, inner_size))
    grid_imag = imag_part.reshape(leading + (radix_split, inner_size))
    outer_cos, outer_sin = angle_tables(radix_split, radix_split, radix_split, direction)
    section_real, section_imag = complex_product(
        "...ab,ak->...kb", grid_real, grid_imag, outer_cos, outer_sin
    )
    twist_cos, twist_sin = angle_tables(radix_split, inner_size, length, direction)
    turned_real = section_real * twist_cos - section_imag * twist_sin
    turned_imag = section_real * twist_sin + section_imag * twist_cos
    inner_cos, inner_sin = angle_tables(inner_size, inner_size, inner_size, direction)
    final_real, final_imag = complex_product(
        "...kb,bm->...mk", turned_real, turned_imag, inner_cos, inner_sin
    )
    return (final_real.reshape(leading + (length,)), final_imag.reshape(leading + (length,)))


def project(lines, wave_x, wave_z, kept_line):
    groups, per_device, length_y = lines.shape
    shaped = lines.reshape(3, 2, groups // 6, per_device, length_y)
    spec_real, spec_imag = transform(shaped[:, 0], shaped[:, 1], -1.0)
    index_y = jnp.arange(length_y)
    signed_y = jnp.where(index_y <= length_y // 2, index_y, index_y - length_y)
    kept_y = jnp.abs(signed_y) <= length_y // 3
    retained = (kept_line & kept_y[None, None, :]).astype(jnp.float32)
    wave_y = signed_y.astype(jnp.float32)[None, None, :]
    wave_square = wave_x * wave_x + wave_y * wave_y + wave_z * wave_z
    waves = (wave_x, wave_y, wave_z)
    div_real = wave_x * spec_real[0] + wave_y * spec_real[1] + wave_z * spec_real[2]
    div_imag = wave_x * spec_imag[0] + wave_y * spec_imag[1] + wave_z * spec_imag[2]
    proj_real = jnp.stack(
        [
            (spec_real[component] - waves[component] * div_real / wave_square) * retained
            for component in range(3)
        ]
    )
    proj_imag = jnp.stack(
        [
            (spec_imag[component] - waves[component] * div_imag / wave_square) * retained
            for component in range(3)
        ]
    )
    back_real, back_imag = transform(proj_real, proj_imag, 1.0)
    return jnp.stack([back_real / length_y, back_imag / length_y], axis=1).reshape(
        groups, per_device, length_y
    )


def first_send(spectrum, first_size):
    groups, rows, span = spectrum.shape
    return (
        spectrum.reshape(groups, rows, first_size, span // first_size)
        .transpose(2, 0, 1, 3)
        .reshape(first_size, 1, -1)
    )


def second_send(received, first_size, second_size, groups, rows, per_device):
    shaped = received.reshape(first_size, groups, rows, second_size, per_device)
    return shaped.transpose(3, 1, 4, 0, 2).reshape(second_size, 1, -1)


def arrange_lines(received, first_size, second_size, groups, rows, per_device):
    shaped = received.reshape(second_size, groups, per_device, first_size, rows)
    ordered = shaped.transpose(1, 2, 0, 3, 4)
    return ordered.reshape(groups, per_device, -1)


def first_return(solved, first_size, second_size, rows):
    groups, per_device, _ = solved.shape
    shaped = solved.reshape(groups, per_device, second_size, first_size, rows).transpose(
        2, 0, 1, 3, 4
    )
    return shaped.reshape(second_size, 1, -1)


def second_return(received, first_size, second_size, groups, rows, per_device):
    shaped = received.reshape(second_size, groups, per_device, first_size, rows)
    return shaped.transpose(3, 1, 4, 0, 2).reshape(first_size, 1, -1)


def arrange_rows(received, first_size, groups, rows):
    shaped = received.reshape(first_size, groups, rows, -1)
    return shaped.transpose(1, 2, 0, 3).reshape(groups, rows, -1)


def local_generic(velocity, plane_wavenumber):
    components, plane_count, row_count, x_length = velocity.shape
    wide_size = lax.axis_size("wide")
    narrow_size = lax.axis_size("narrow")
    device_count = wide_size * narrow_size
    keep_x = x_length // 3 + 1
    spec_real, spec_imag = transform(velocity, jnp.zeros_like(velocity), -1.0)
    spec_real = spec_real[..., :keep_x]
    spec_imag = spec_imag[..., :keep_x]
    per_device = (keep_x + device_count - 1) // device_count
    line_span = per_device * device_count
    gap = ((0, 0), (0, 0), (0, 0), (0, 0), (0, line_span - keep_x))
    stacked = jnp.stack([spec_real, spec_imag], axis=1)
    spectrum = jnp.pad(stacked, gap).reshape(components * 2 * plane_count, row_count, line_span)
    groups = spectrum.shape[0]
    halfway = lax.all_to_all(
        first_send(spectrum, narrow_size), "narrow", split_axis=0, concat_axis=1, tiled=True
    )
    outgoing = second_send(halfway, narrow_size, wide_size, groups, row_count, per_device)
    arrived = lax.all_to_all(outgoing, "wide", split_axis=0, concat_axis=1, tiled=True)
    lines = arrange_lines(arrived, narrow_size, wide_size, groups, row_count, per_device)
    line_start = (
        lax.axis_index("narrow") * (per_device * wide_size) + lax.axis_index("wide") * per_device
    )
    indices = line_start + jnp.arange(per_device)
    wave_x = indices.astype(jnp.float32)[None, :, None]
    wave_z = plane_wavenumber[:, None, None]
    kept_line = (indices < keep_x)[None, :, None]
    solved = project(lines, wave_x, wave_z, kept_line)
    halfway = lax.all_to_all(
        first_return(solved, narrow_size, wide_size, row_count),
        "wide",
        split_axis=0,
        concat_axis=1,
        tiled=True,
    )
    outgoing = second_return(halfway, narrow_size, wide_size, groups, row_count, per_device)
    arrived = lax.all_to_all(outgoing, "narrow", split_axis=0, concat_axis=1, tiled=True)
    returned = arrange_rows(arrived, narrow_size, groups, row_count)
    columns = returned.reshape(components, 2, plane_count, row_count, line_span)[..., :keep_x]
    weights = jnp.where(jnp.arange(keep_x) == 0, 1.0, 2.0).astype(jnp.float32)
    widen = ((0, 0), (0, 0), (0, 0), (0, x_length - keep_x))
    back_real = jnp.pad(columns[:, 0] * weights, widen)
    back_imag = jnp.pad(columns[:, 1] * weights, widen)
    out_real, _ = transform(back_real, back_imag, 1.0)
    return out_real / x_length


radix = 16
lane = 128
tile = 8
axes = ("wide", "narrow")


def split_parts(values):
    high = values.astype(jnp.bfloat16)
    low = (values - high.astype(jnp.float32)).astype(jnp.bfloat16)
    return high, low


def split_table(values):
    values = values.astype(np.float32)
    high = values.astype(jnp.bfloat16)
    low = (values - high.astype(np.float32)).astype(jnp.bfloat16)
    return high, low


def turns(product, period):
    angle = 2.0 * np.pi * (np.asarray(product) % period) / period
    return np.cos(angle), np.sin(angle)


def twist_table(inner):
    return turns(np.arange(radix)[:, None] * np.arange(inner)[None, :], radix * inner)


def line_chunks(per_device):
    first = per_device // (4 * tile) * (2 * tile)
    last = per_device - first
    main = last // tile * tile
    return ((0, first, first, 2 * first), (first, last, main, 2 * main + tile))


def line_slots(per_device):
    half = tile // 2
    base = 0
    slots = []
    for start, lines, main, height in line_chunks(per_device):
        slots += [(base + line, start + line, 0) for line in range(main)]
        slots += [(base + main + line, start + line, 1) for line in range(main)]
        for extra in range(lines - main):
            slots.append((base + 2 * main + extra, start + main + extra, 0))
            slots.append((base + 2 * main + half + extra, start + main + extra, 1))
        base += height
    return slots


def row_table(inner, per_device, shares, block):
    rows = np.zeros((2 * shares * block, 2 * inner))
    points = np.arange(inner)
    for share in range(shares):
        for row, line, part in line_slots(per_device):
            q = share * per_device + line
            cos, sin = turns(q * points, inner)
            rows[share * block + row] = np.concatenate([-sin, cos] if part else [cos, sin])
            cos, sin = turns((q + 1) * points, inner)
            rows[(shares + share) * block + row] = np.concatenate([-sin, -cos] if part else [cos, -sin])
    return rows


def square_table(inner):
    cos, sin = turns(np.arange(inner)[:, None] * np.arange(inner)[None, :], inner)
    return np.block([[cos, -sin], [sin, cos]])


def scaled(value, cos, sin):
    real, imag = value
    if abs(sin) < 1e-12:
        return (real, imag) if cos > 0 else (-real, -imag)
    if abs(cos) < 1e-12:
        return (-imag, real) if sin > 0 else (imag, -real)
    if abs(abs(cos) - abs(sin)) < 1e-12:
        size = abs(cos)
        a, b = (1.0 if cos > 0 else -1.0), (1.0 if sin > 0 else -1.0)
        first = (real if a > 0 else -real) + (-imag if b > 0 else imag)
        second = (real if b > 0 else -real) + (imag if a > 0 else -imag)
        return first * size, second * size
    return real * cos - imag * sin, real * sin + imag * cos


def unit(step, size, direction):
    angle = direction * 2.0 * math.pi * step / size
    return math.cos(angle), math.sin(angle)


def complex_fft(values, direction):
    size = len(values)
    if size == 1:
        return values
    even = complex_fft(values[0::2], direction)
    odd = complex_fft(values[1::2], direction)
    first, second = [], []
    for k in range(size // 2):
        real, imag = scaled(odd[k], *unit(k, size, direction))
        first.append((even[k][0] + real, even[k][1] + imag))
        second.append((even[k][0] - real, even[k][1] - imag))
    return first + second


def real_fft(values):
    size = len(values)
    if size == 2:
        return [(values[0] + values[1], None), (values[0] - values[1], None)]
    even = real_fft(values[0::2])
    odd = real_fft(values[1::2])
    quarter = size // 4
    out = [None] * (size // 2 + 1)
    out[0] = (even[0][0] + odd[0][0], None)
    out[size // 2] = (even[0][0] - odd[0][0], None)
    for k in range(1, quarter):
        real, imag = scaled(odd[k], *unit(k, size, -1.0))
        out[k] = (even[k][0] + real, even[k][1] + imag)
        out[size // 2 - k] = (even[k][0] - real, imag - even[k][1])
    out[quarter] = (even[quarter][0], -odd[quarter][0])
    return out


def real_sum(values):
    count = len(values) - 1
    size = 2 * count
    if size == 2:
        return [values[0][0] + values[1][0], values[0][0] - values[1][0]]
    half = count // 2
    even = [(values[0][0] + values[count][0], None)]
    odd = [(values[0][0] - values[count][0], None)]
    for s in range(1, half):
        near, far = values[s], values[count - s]
        even.append((near[0] + far[0], near[1] - far[1]))
        odd.append(scaled((near[0] - far[0], near[1] + far[1]), *unit(s, size, 1.0)))
    even.append((values[half][0], None))
    odd.append((-values[half][1], None))
    even_out, odd_out = real_sum(even), real_sum(odd)
    out = []
    for m in range(count):
        out += [even_out[m], odd_out[m]]
    return out


def three_products(left, right, dims):
    left_high, left_low = left
    right_high, right_low = right

    def one(a, b):
        return lax.dot_general(a, b, (dims, ((), ())), preferred_element_type=jnp.float32)

    return one(left_high, right_high) + one(left_low, right_high) + one(left_high, right_low)


def stacked_products(stack_ref, height, high, low):
    depth = stack_ref.shape[0] // 2

    def one(a, b):
        return lax.dot_general(a, b, (((1,), (1,)), ((), ())), preferred_element_type=jnp.float32)

    if 2 * height < depth:
        upper, lower = one(stack_ref[:height], high), one(stack_ref[depth : depth + height], high)
    else:
        both = one(stack_ref[...], high)
        upper, lower = both[:height], both[depth : depth + height]
    return upper + lower + one(stack_ref[:height], low)


def slot_order():
    return [0, radix // 2] + list(range(1, radix // 2))


def rows_forward(
    index_ref, x_ref, stack_ref, cos_ref, sin_ref, near_ref, *refs, shares, block
):
    far_refs = refs[:-3]
    th_ref, tl_ref, box_ref = refs[-3:]
    split = near_ref.shape[1]
    rows, length = x_ref.shape[2:]
    inner = length // radix
    order = slot_order()
    chunk = 2 * tile

    def vector_stage(step, carry):
        start = pl.multiple_of(step * chunk, chunk)
        for column in range(0, inner, lane):
            parts = [
                x_ref[0, 0, pl.ds(start, chunk), a * inner + column : a * inner + column + lane]
                for a in range(radix)
            ]
            spectrum = real_fft(parts)
            for slot, s in enumerate(order):
                real, imag = spectrum[s]
                if s:
                    cos = cos_ref[s : s + 1, column : column + lane]
                    sin = sin_ref[s : s + 1, column : column + lane]
                    if imag is None:
                        real, imag = real * cos, -(real * sin)
                    else:
                        real, imag = real * cos + imag * sin, imag * cos - real * sin
                else:
                    imag = jnp.zeros_like(real)
                where = pl.ds(pl.multiple_of(slot * rows + start, chunk), chunk)
                for offset, part in ((0, real), (inner, imag)):
                    high, low = split_parts(part)
                    th_ref[where, offset + column : offset + column + lane] = high
                    tl_ref[where, offset + column : offset + column + lane] = low
        return carry

    lax.fori_loop(0, rows // chunk, vector_stage, 0)
    single = shares * block
    slot = 0
    while slot < len(order):
        count = min(2, len(order) - slot)
        height = single if slot == 0 else 2 * single
        where = slice(slot * rows, (slot + count) * rows)
        result = stacked_products(stack_ref, height, th_ref[where], tl_ref[where])
        for index in range(count):
            s = order[slot + index]
            columns = result[:, index * rows : (index + 1) * rows]
            for share in range(shares):
                targets = [(s, share)] + ([(radix - s, shares + share)] if slot else [])
                for residue, position in targets:
                    piece = columns[position * block : (position + 1) * block]
                    near_ref[residue * shares + share] = piece[:split]
                    box_ref[residue * shares + share] = piece[split:]
        slot += count
    height = block - split
    where = pl.ds(pl.program_id(0) * height, height)
    for k, far_ref in enumerate(far_refs):
        far_ref[where, :] = box_ref[index_ref[0] ^ k]


def rows_back(index_ref, near_ref, stack_ref, cos_ref, sin_ref, *refs, shares, block):
    out_ref, g_ref, far_ref = refs[-3:]
    devices, height = far_ref.shape[:2]
    place = pl.ds(pl.program_id(0) * height, height)
    for k in range(devices):
        far_ref[index_ref[0] ^ k] = refs[k][place, :]
    rows, length = out_ref.shape[2:]
    inner = length // radix
    order = slot_order()
    depth = stack_ref.shape[0] // 2
    for slot, s in enumerate(order):
        blocks = []
        for residue in [s] if slot < 2 else [s, radix - s]:
            for share in range(shares):
                blocks += [near_ref[residue * shares + share], far_ref[residue * shares + share]]
        used = len(blocks) // 2 * block
        wide = -(-used // lane) * lane
        if wide > used:
            blocks.append(jnp.zeros((wide - used, rows), jnp.float32))
        turned = jnp.transpose(jnp.concatenate(blocks, axis=0))
        g_ref[slot * rows : (slot + 1) * rows] = three_products(
            split_parts(turned), (stack_ref[:wide], stack_ref[depth : depth + wide]), ((1,), (0,))
        )
    chunk = 2 * tile

    def vector_stage(step, carry):
        start = pl.multiple_of(step * chunk, chunk)
        for column in range(0, inner, lane):
            values = [None] * len(order)
            for slot, s in enumerate(order):
                where = pl.ds(pl.multiple_of(slot * rows + start, chunk), chunk)
                real = g_ref[where, column : column + lane]
                if s:
                    imag = g_ref[where, inner + column : inner + column + lane]
                    cos = cos_ref[s : s + 1, column : column + lane]
                    sin = sin_ref[s : s + 1, column : column + lane]
                    if 2 * s == radix:
                        real, imag = real * cos - imag * sin, None
                    else:
                        real, imag = real * cos - imag * sin, real * sin + imag * cos
                else:
                    imag = None
                values[s] = (real, imag)
            for a, out in enumerate(real_sum(values)):
                out_ref[0, 0, pl.ds(start, chunk), a * inner + column : a * inner + column + lane] = out
        return carry

    lax.fori_loop(0, rows // chunk, vector_stage, 0)


def lines_middle(
    index_ref, wave_ref, *refs, counts, targets, shares, chunk_shape, per_device, keep_x, length_x
):
    in_refs = refs[: len(counts)]
    high_ref, low_ref, cos_ref, sin_ref = refs[len(counts) : len(counts) + 4]
    th_ref, tl_ref, x_ref = refs[-3:]
    out_refs = refs[-3 - len(targets) : -3]
    first, lines, main, block = chunk_shape
    components = sum(counts)
    rows = in_refs[0].shape[2]
    inner = shares * rows
    length_y = radix * inner
    chunk = 2 * tile
    padded = -(-lines // chunk) * chunk
    half = tile // 2

    def read(in_ref, c, source, start):
        real, imag = [], []
        for row in range(start, start + chunk, tile):
            if row < main:
                real.append(in_ref[source, pl.ds(c * block + row, tile), :])
                imag.append(in_ref[source, pl.ds(c * block + main + row, tile), :])
            elif row == main:
                last = in_ref[source, pl.ds(c * block + 2 * main, tile), :]
                real.append(last)
                imag.append(pltpu.roll(last, half, 0))
            else:
                real.append(jnp.zeros((tile, rows), jnp.float32))
                imag.append(jnp.zeros((tile, rows), jnp.float32))
        return jnp.concatenate(real, axis=0), jnp.concatenate(imag, axis=0)

    def write(out_ref, c, target, start, real, imag):
        for position, row in enumerate(range(start, start + chunk, tile)):
            a = real[position * tile : (position + 1) * tile]
            b = imag[position * tile : (position + 1) * tile]
            if row < main:
                out_ref[target, pl.ds(c * block + row, tile), :] = a
                out_ref[target, pl.ds(c * block + main + row, tile), :] = b
            elif row == main:
                index = lax.broadcasted_iota(jnp.int32, (tile, rows), 0)
                out_ref[target, pl.ds(c * block + 2 * main, tile), :] = jnp.where(
                    index < half, a, pltpu.roll(b, half, 0)
                )

    def forward(in_ref, base, position, carry):
        c = base + position
        for start in range(0, padded, chunk):
            for share in range(shares):
                column = share * rows
                values = [
                    read(in_ref, position, a * shares + share, start) for a in range(radix)
                ]
                for s, (real, imag) in enumerate(complex_fft(values, -1.0)):
                    if s:
                        cos = cos_ref[s : s + 1, column : column + rows]
                        sin = sin_ref[s : s + 1, column : column + rows]
                        real, imag = real * cos + imag * sin, imag * cos - real * sin
                    where = slice(s * padded + start, s * padded + start + chunk)
                    for offset, part in ((0, real), (inner, imag)):
                        high, low = split_parts(part)
                        th_ref[c, where, offset + column : offset + column + rows] = high
                        tl_ref[c, where, offset + column : offset + column + rows] = low
        return carry

    base = 0
    for in_ref, count in zip(in_refs, counts):
        lax.fori_loop(0, count, functools.partial(forward, in_ref, base), 0)
        base += count

    def products(dims):
        def run(c, carry):
            x_ref[c] = three_products(
                (th_ref[c], tl_ref[c]), (high_ref[...], low_ref[...]), dims
            )
            return carry

        lax.fori_loop(0, components, run, 0)

    products(((1,), (0,)))

    share_of = index_ref[0] % shares
    offset_of = index_ref[0] // shares
    wave_z = wave_ref[0]
    scale = 1.0 / (length_x * length_y)

    def middle(s, carry):
        for start in range(0, padded, chunk):
            line = lax.broadcasted_iota(jnp.int32, (chunk, inner), 0) + start
            line_x = (share_of * per_device + first + line) * radix + offset_of
            index_y = lax.broadcasted_iota(jnp.int32, (chunk, inner), 1) * radix + s
            signed_y = jnp.where(index_y <= length_y // 2, index_y, index_y - length_y)
            kept = (line < lines) & (line_x < keep_x) & (jnp.abs(signed_y) <= length_y // 3)
            weight = jnp.where(line_x == 0, scale, 2.0 * scale)
            factor = jnp.where(kept, weight, 0.0)
            wave_x = line_x.astype(jnp.float32)
            wave_y = signed_y.astype(jnp.float32)
            waves = (wave_x, wave_y, wave_z)
            inverse = factor / (wave_x * wave_x + wave_y * wave_y + wave_z * wave_z)
            where = pl.ds(pl.multiple_of(s * padded + start, chunk), chunk)
            for offset in (0, inner):
                columns = slice(offset, offset + inner)
                values = [x_ref[c, where, columns] for c in range(components)]
                divergence = (
                    wave_x * values[0] + wave_y * values[1] + wave_z * values[2]
                ) * inverse
                for c in range(components):
                    high, low = split_parts(factor * values[c] - waves[c] * divergence)
                    th_ref[c, where, columns] = high
                    tl_ref[c, where, columns] = low
        return carry

    lax.fori_loop(0, radix, middle, 0)
    products(((1,), (1,)))

    def backward(out_ref, base, position, carry):
        c = base + position
        for start in range(0, padded, chunk):
            for share in range(shares):
                column = share * rows
                values = []
                for s in range(radix):
                    where = slice(s * padded + start, s * padded + start + chunk)
                    real = x_ref[c, where, column : column + rows]
                    imag = x_ref[c, where, inner + column : inner + column + rows]
                    if s:
                        cos = cos_ref[s : s + 1, column : column + rows]
                        sin = sin_ref[s : s + 1, column : column + rows]
                        real, imag = real * cos - imag * sin, real * sin + imag * cos
                    values.append((real, imag))
                for a, (real, imag) in enumerate(complex_fft(values, 1.0)):
                    write(out_ref, position, a * shares + share, start, real, imag)
        return carry

    base = 0
    for out_ref, count in zip(out_refs, targets):
        lax.fori_loop(0, count, functools.partial(backward, out_ref, base), 0)
        base += count


def whole(shape):
    return pl.BlockSpec(shape, lambda *_: (0,) * len(shape))


def token_of(in_ref, out_ref):
    out_ref[...] = in_ref[0]


def exchange(values):
    return lax.all_to_all(values, axes, split_axis=0, concat_axis=0, tiled=True)


def swap(blocks):
    count = len(blocks)
    moved = list(blocks)
    for k in range(1, count):
        moved[k] = lax.ppermute(blocks[k], axes, [(source, source ^ k) for source in range(count)])
    return moved


def local_fast(velocity, plane_wavenumber):
    components, _, rows, length_x = velocity.shape
    devices = lax.axis_size("wide") * lax.axis_size("narrow")
    keep_x = length_x // 3 + 1
    inner = length_x // radix
    shares = devices // radix
    per_device = -(-keep_x // (radix * shares))
    near, far = line_chunks(per_device)
    block = near[3] + far[3]
    table = row_table(inner, per_device, shares, block)
    table = np.pad(table, ((0, -len(table) % lane), (0, 0)))
    line_inner = shares * rows
    row_tables = [jnp.asarray(np.concatenate(split_table(table)))]
    row_tables += [jnp.asarray(t, jnp.float32) for t in twist_table(inner)]
    line_tables = [jnp.asarray(t) for t in split_table(square_table(line_inner))]
    line_tables += [jnp.asarray(t, jnp.float32) for t in twist_table(line_inner)]
    limits = pltpu.CompilerParams(vmem_limit_bytes=56 * 1024 * 1024)
    slots = radix // 2 + 1
    anywhere = pl.BlockSpec(memory_space=pl.ANY)
    scalar = pl.BlockSpec(memory_space=pltpu.SMEM)
    index = lax.axis_index(axes).astype(jnp.int32).reshape(1)

    def shape(count, height):
        return jax.ShapeDtypeStruct((devices, count * height, rows), jnp.float32)

    def single(count):
        return jax.ShapeDtypeStruct((count * far[3], rows), jnp.float32)

    def box(count):
        return pltpu.VMEM((devices, count * far[3], rows), jnp.float32)

    def component(height):
        return pl.BlockSpec((devices, height, rows), lambda c: (0, c, 0))

    field = pl.BlockSpec((1, 1, rows, length_x), lambda c: (c, 0, 0, 0))

    near_lines, *far_lines = pl.pallas_call(
        functools.partial(rows_forward, shares=shares, block=block),
        grid=(components,),
        in_specs=[scalar, field] + [whole(t.shape) for t in row_tables],
        out_specs=[component(near[3])] + [whole(single(components).shape)] * devices,
        out_shape=[shape(components, near[3])] + [single(components)] * devices,
        scratch_shapes=[pltpu.VMEM((slots * rows, 2 * inner), jnp.bfloat16)] * 2 + [box(1)],
        compiler_params=limits,
        name="rows_forward",
    )(index, velocity, *row_tables)

    def middle(sources, targets, chunk_shape):
        spread = len(sources) > 1
        height = chunk_shape[3]
        padded = -(-chunk_shape[1] // (2 * tile)) * 2 * tile
        group = (components, radix * padded, 2 * line_inner)
        outs = [shape(count, height) for count in targets]
        if spread:
            outs = outs[:-1] + [single(targets[-1])] * devices
        place = 2 + len(sources) + len(line_tables)

        def body(*refs):
            index_ref, wave_ref = refs[:2]
            from_refs, tables = refs[2 : 2 + len(sources)], refs[2 + len(sources) : place]
            to_refs, scratch = refs[place : place + len(outs)], refs[place + len(outs) :]
            spread_refs = to_refs[-devices:]
            if spread:
                in_box, out_box, *scratch = scratch
                for k, ref in enumerate(from_refs):
                    in_box[index_ref[0] ^ k] = ref[...]
                from_refs, to_refs = [in_box], to_refs[:-devices] + (out_box,)
            lines_middle(
                index_ref, wave_ref, *from_refs, *tables, *to_refs, *scratch, counts=(components,),
                targets=targets, shares=shares, chunk_shape=chunk_shape, per_device=per_device,
                keep_x=keep_x, length_x=length_x,
            )
            if spread:
                for k, ref in enumerate(spread_refs):
                    ref[...] = out_box[index_ref[0] ^ k]

        return pl.pallas_call(
            body,
            grid=(1,),
            in_specs=[scalar, scalar]
            + [whole(t.shape) for t in sources]
            + [whole(t.shape) for t in line_tables],
            out_specs=[whole(t.shape) for t in outs],
            out_shape=outs,
            scratch_shapes=([box(components), box(targets[-1])] if spread else [])
            + [pltpu.VMEM(group, jnp.bfloat16)] * 2
            + [pltpu.VMEM(group, jnp.float32)],
            compiler_params=limits,
        )(index, plane_wavenumber, *sources, *line_tables)

    def back(near_lines, far_lines, token):
        return pl.pallas_call(
            functools.partial(rows_back, shares=shares, block=block),
            grid=(components,),
            in_specs=[scalar, component(near[3])]
            + [whole(t.shape) for t in row_tables]
            + [whole(single(components).shape)] * devices
            + [anywhere],
            out_specs=field,
            out_shape=jax.ShapeDtypeStruct(velocity.shape, jnp.float32),
            scratch_shapes=[pltpu.VMEM((slots * rows, 2 * inner), jnp.float32), box(1)],
            compiler_params=limits,
            name="rows_back",
        )(index, near_lines, *row_tables, *far_lines, token)

    near_lines = exchange(near_lines)
    far_lines = swap(far_lines)
    (near_lines,) = middle([near_lines], (components,), near)
    near_lines = exchange(near_lines)
    far_lines = middle(far_lines, (components,), far)
    far_lines = swap(far_lines)
    token = pl.pallas_call(
        token_of,
        grid=(1,),
        in_specs=[pl.BlockSpec((1, tile, lane), lambda _: (0, 0, 0))],
        out_specs=whole((tile, lane)),
        out_shape=jax.ShapeDtypeStruct((tile, lane), jnp.float32),
        name="near_token",
    )(near_lines)
    return back(near_lines, far_lines, token)


def local(velocity, plane_wavenumber):
    components, planes, rows, length_x = velocity.shape
    devices = lax.axis_size("wide") * lax.axis_size("narrow")
    keep_x = length_x // 3 + 1
    fits = (
        components == 3
        and planes == 1
        and rows == lane
        and length_x % (radix * lane) == 0
        and devices % radix == 0
        and devices & (devices - 1) == 0
        and -(-keep_x // devices) == -(-(-(-keep_x // radix)) // (devices // radix))
        and -(-keep_x // devices) % tile <= tile // 2
        and (rows * devices) // 3 < rows * devices // 2
    )
    if fits:
        return local_fast(velocity, plane_wavenumber)
    return local_generic(velocity, plane_wavenumber)


def solution(mesh):
    placed = (P(None, None, ("wide", "narrow"), None), P())

    return jax.shard_map(
        local,
        mesh=mesh,
        in_specs=placed,
        out_specs=P(None, None, ("wide", "narrow"), None),
        check_vma=False,
    )
```
